32 devices in a mesh: leaf: 8 (over z, y), rhs: 4 (over x, core).
Axes of the slice: x: 2, y: 2, z: 4, core: 2. Of those that a mesh axis runs over, the one named last changes fastest.
Arguments:
- right_sides: float32 [64, 8192], P('rhs', 'leaf'), may hold values from -8 to 8
- leaf_inverse: float32 [8192, 1024], P('leaf', 'rhs'), may hold values from -1 to 5, as said below
- bases: bfloat16 [3, 128, 8192], P(None, None, 'leaf'), may hold values from -1 to 1
- ordering: int32 [8, 1024], P('leaf'), may hold values from 0 to 1023, as said below
Outputs:
- solution: float32 [64, 8192], P('rhs', 'leaf')
The draws below stay inside these ranges and needn't reach their ends.
Inputs may be any that keep to these rules, and one draw needn't show every extreme that they name: `leaf_inverse`: each leaf's block of 1024 rows is symmetric positive definite. `ordering`: each row is a permutation of 0 to 1023.
All inputs are finite; a program needn't handle non-finite values.
Results may differ from the reference program's by a relative error of at most 0.0003.
Values sent between devices are 32-bit elements; how exact they have to be, the bound alone decides.
A program may use at most 64 MiB of HBM per device.

```python
import math
import jax
import jax.numpy as jnp
from jax import lax

LEAF = 1024
R = 128
RHS = 64
LEVELS = 3
NPTS = 8192
N_LEAF = 8


def basis_and_order(key):
    order_key = jax.random.fold_in(key, 7)
    leaf_keys = jax.random.split(order_key, N_LEAF)
    ordering = jax.vmap(lambda single: jax.random.permutation(single, LEAF))(leaf_keys).astype(jnp.int32)
    noise_key = jax.random.fold_in(key, 11)
    heights = jnp.arange(1, LEVELS + 1, dtype=jnp.float32)
    scales = 2.0 / jnp.sqrt(LEAF * 2.0 ** heights)
    noise = jax.random.normal(noise_key, (LEVELS, R, NPTS))
    basis_rows = jnp.clip(noise * scales[:, None, None], -1.0, 1.0)
    return (basis_rows, ordering)


def draw_bases(key, part):
    return basis_and_order(key)[0].astype(jnp.bfloat16)


def draw_ordering(key, part):
    return basis_and_order(key)[1]


def draw_right_sides(key, part):
    basis_rows, ordering = basis_and_order(key)
    tree_order = jnp.zeros((RHS, NPTS), jnp.float32)
    for height in range(LEVELS):
        node_span = LEAF * 2 ** (height + 1)
        groups = NPTS // node_span
        spread = (node_span / (4.0 * R)) ** 0.5
        mixing = jax.random.normal(jax.random.fold_in(key, 40 + height), (groups, R, RHS)) * spread
        level_term = jnp.einsum('rns,nrk->kns', basis_rows[height].reshape(R, groups, node_span), mixing)
        tree_order = tree_order + level_term.reshape(RHS, NPTS)
    tree_order = 0.5 * tree_order + 0.5 * jax.random.normal(jax.random.fold_in(key, 50), (RHS, NPTS))
    tree_order = jnp.clip(tree_order, -8.0, 8.0)
    by_leaf = tree_order.reshape(RHS, N_LEAF, LEAF)
    leaf_ids = jnp.arange(N_LEAF, dtype=jnp.int32)[:, None]
    data_order = jnp.zeros_like(by_leaf).at[:, leaf_ids, ordering].set(by_leaf)
    return data_order.reshape(RHS, NPTS)


def draw_leaf_inverse(key, part):
    diag_key = jax.random.fold_in(key, 21)
    off_key = jax.random.fold_in(key, 22)
    diagonal = jnp.exp(jax.random.uniform(diag_key, (N_LEAF, LEAF), minval=math.log(0.5), maxval=math.log(2.0)))
    raw_values = jnp.clip(jax.random.normal(off_key, (N_LEAF, LEAF, LEAF)), -3.0, 3.0)
    off_part = (raw_values + jnp.transpose(raw_values, (0, 2, 1))) * (0.2 / math.sqrt(2.0 * LEAF))
    matrix = off_part + diagonal[:, :, None] * jnp.eye(LEAF, dtype=jnp.float32)
    return jnp.clip(matrix, -1.0, 5.0).reshape(NPTS, LEAF)


def setup_inputs(seed: int = 0) -> dict:
    splits = jax.random.split(jax.random.key(seed), 5)
    return {
        "right_sides": draw_right_sides(jax.random.fold_in(splits[4], 71), 0),
        "leaf_inverse": draw_leaf_inverse(jax.random.fold_in(splits[4], 71), 0),
        "bases": draw_bases(jax.random.fold_in(splits[4], 71), 0),
        "ordering": draw_ordering(jax.random.fold_in(splits[4], 71), 0),
    }


def solve_factor(factor, values):
    middle = lax.linalg.triangular_solve(factor, values, left_side=True, lower=True)
    return lax.linalg.triangular_solve(factor, middle, left_side=True, lower=True, transpose_a=True)

def reference(right_sides, leaf_inverse, bases, ordering):
    highest = lax.Precision.HIGHEST
    by_leaf = right_sides.reshape(RHS, N_LEAF, LEAF)
    tree_order = jnp.take_along_axis(by_leaf, ordering[None, :, :], axis=2)
    basis_rows = bases.astype(jnp.float32)
    stacked = jnp.concatenate([tree_order, basis_rows.reshape(LEVELS * R, N_LEAF, LEAF)], 0)
    inverses = leaf_inverse.reshape(N_LEAF, LEAF, LEAF)
    applied = jnp.einsum('cip,iqp->ciq', stacked, inverses, precision=highest)
    applied = applied.reshape(RHS + LEVELS * R, NPTS)
    solved = applied[:RHS]
    pending = [applied[RHS + offset * R:RHS + (offset + 1) * R] for offset in range(LEVELS)]
    for height in range(LEVELS):
        node_span = LEAF * 2 ** (height + 1)
        groups = NPTS // node_span
        level_basis = basis_rows[height].reshape(R, groups, node_span)
        level_solved = pending[height].reshape(R, groups, node_span)
        carried = jnp.concatenate([solved] + pending[height + 1:], 0)
        column_count = carried.shape[0]
        grouped = carried.reshape(column_count, groups, node_span)
        capacity = jnp.einsum('rgp,sgp->grs', level_basis, level_solved, precision=highest)
        capacity = capacity + jnp.eye(R, dtype=jnp.float32)
        projected = jnp.einsum('rgp,cgp->grc', level_basis, grouped, precision=highest)
        factor = jnp.linalg.cholesky(capacity)
        weights = solve_factor(factor, projected)
        grouped = grouped - jnp.einsum('grc,rgp->cgp', weights, level_solved, precision=highest)
        carried = grouped.reshape(column_count, NPTS)
        solved = carried[:RHS]
        later = [carried[RHS + offset * R:RHS + (offset + 1) * R] for offset in range(LEVELS - height - 1)]
        pending = pending[:height + 1] + later
    untangled = solved.reshape(RHS, N_LEAF, LEAF)
    leaf_ids = jnp.arange(N_LEAF, dtype=jnp.int32)[:, None]
    result = jnp.zeros_like(untangled).at[:, leaf_ids, ordering].set(untangled)
    return result.reshape(RHS, NPTS)
```

```python
import functools

import jax
import jax.numpy as jnp
from jax import lax
from jax.experimental import pallas as pl
from jax.experimental.pallas import tpu as pltpu
from jax.sharding import PartitionSpec as P

F32 = jnp.float32
BF16 = jnp.bfloat16
NN = (((1,), (0,)), ((), ()))
NT = (((1,), (1,)), ((), ()))
STEP = 8


def split(value, pieces):
    parts = []
    for _ in range(pieces):
        head = value.astype(BF16)
        parts.append(head)
        value = value - head.astype(F32)
    return parts


def dot(left, right, dims):
    return lax.dot_general(left, right, dims, preferred_element_type=F32)


def fine(left, right, dims):
    return lax.dot_general(
        left, right, dims, precision=lax.Precision.HIGHEST, preferred_element_type=F32
    )


def inverse(matrix):
    size = matrix.shape[0]
    lane = lax.broadcasted_iota(jnp.int32, (1, size), 1)
    row_of = lax.broadcasted_iota(jnp.int32, (STEP, 1), 0)

    def block(_, a):
        for k in range(0, STEP, 2):
            first, second = a[k : k + 1], a[k + 1 : k + 2]
            a00 = jnp.broadcast_to(a[k : k + 1, k : k + 1], (1, size))
            a01 = jnp.broadcast_to(a[k : k + 1, k + 1 : k + 2], (1, size))
            a10 = jnp.broadcast_to(a[k + 1 : k + 2, k : k + 1], (1, size))
            a11 = jnp.broadcast_to(a[k + 1 : k + 2, k + 1 : k + 2], (1, size))
            scale = 1.0 / (a00 * a11 - a01 * a10)
            at0, at1 = lane == k, lane == k + 1
            first = jnp.where(at0, 1.0, jnp.where(at1, 0.0, first))
            second = jnp.where(at0, 0.0, jnp.where(at1, 1.0, second))
            new0 = (a11 * first - a01 * second) * scale
            new1 = (a00 * second - a10 * first) * scale
            col0, col1 = a[:, k : k + 1], a[:, k + 1 : k + 2]
            kept = jnp.where(at0 | at1, 0.0, a)
            a = kept - col0 * new0 - col1 * new1
            top = jnp.where(row_of == k, new0, jnp.where(row_of == k + 1, new1, a[:STEP]))
            a = jnp.concatenate([top, a[STEP:]], 0)
        a = jnp.concatenate([a[STEP:], a[:STEP]], 0)
        return pltpu.roll(a, size - STEP, 1)

    return lax.fori_loop(0, size // STEP, block, matrix)


def plan(leaves, groups, levels, rank, rows):
    units = [("c0", rank)]
    for j in range(levels):
        height = (levels - j) * rank - (rank if j == 0 else 0)
        if height:
            units.append((f"m{j}", height))
    units.append(("t", levels * rows))
    return units


def other(index, bit):
    return index + bit - 2 * bit * ((index // bit) % 2)


def kernel(cfg, rs_ref, g_ref, b_ref, ord_ref, out_ref, *scratch):
    leaves, groups, levels, rank, own_rows, points, piece = cfg
    rows = groups * own_rows
    units = plan(leaves, groups, levels, rank, rows)
    names = [name for name, _ in units]
    ref = dict(zip(scratch_names(cfg), scratch))
    leaf, position = lax.axis_index("leaf"), lax.axis_index("rhs")
    mesh_id = pl.DeviceIdType.MESH

    def at(leaf_index, rhs_index):
        return {"leaf": leaf_index, "rhs": rhs_index}

    rhs_peers = [lax.rem(position + k, groups) for k in range(1, groups)]
    mate = other(position, 1)
    half = lax.rem(position, 2)
    chips = [(leaf, lax.rem(position + k, groups)) for k in range(2, groups, 2)]
    chips += [(other(leaf, 1), lax.rem(position + k, groups)) for k in range(0, groups, 2)]
    greeted = [(leaf, p) for p in rhs_peers]
    greeted += chips[groups // 2 - 1 :]
    greeted += [(other(leaf, 1 << h), position) for h in range(1, levels)]

    barrier = pltpu.get_barrier_semaphore()
    for target in greeted:
        pl.semaphore_signal(barrier, inc=1, device_id=at(*target), device_id_type=mesh_id)

    def remote(src, dst, sems, slot, target):
        return pltpu.make_async_remote_copy(
            src_ref=src,
            dst_ref=dst,
            send_sem=ref[sems + "_s"].at[slot],
            recv_sem=ref[sems + "_r"].at[slot],
            device_id=at(*target),
            device_id_type=mesh_id,
        )

    g_parts = split(g_ref[...], 3)
    bases = b_ref[...].reshape(levels * rank, points)
    solved = dot(bases, g_parts[0], NN) + (dot(bases, g_parts[1], NN) + dot(bases, g_parts[2], NN))
    ref["y"][...] = solved
    own_cols = pl.ds(pl.multiple_of(position * piece, piece), piece)
    bases_own = b_ref[:, :, own_cols].reshape(levels * rank, piece)
    gram = sum(dot(part, bases_own, NT) for part in reversed(split(solved, 3)))
    for j in range(levels):
        column = gram[j * rank :, j * rank : (j + 1) * rank]
        if j == 0:
            ref["part_c0"][...] = column[:rank]
            column = column[rank:]
        if column.shape[0]:
            ref[f"part_m{j}"][...] = column

    pl.semaphore_wait(barrier, len(greeted))

    def halves(buffer, which):
        count = buffer.shape[0] // 2
        return buffer.at[pl.ds(pl.multiple_of(which * count, count), count)]

    def fold_start(name):
        slot = names.index(name)
        copy = remote(
            halves(ref["part_" + name], 1 - half), ref["fold_" + name], "fold", slot, (leaf, mate)
        )
        copy.start()
        return copy

    def spread_start(name, fold):
        fold.wait_recv()
        slot = names.index(name)
        ref["chip_" + name][...] = halves(ref["part_" + name], half)[...] + ref["fold_" + name][...]
        copies = []
        for k, target in enumerate(chips):
            copy = remote(
                ref["chip_" + name],
                ref["peer_" + name].at[k],
                "peer",
                slot * len(chips) + k,
                target,
            )
            copy.start()
            copies.append(copy)
        return copies

    def join_start(name, copies):
        for copy in copies:
            copy.wait_recv()
        total = ref["chip_" + name][...]
        for k in range(len(copies)):
            total = total + ref["peer_" + name][k]
        halves(ref["full_" + name], half)[...] = total
        slot = names.index(name)
        copy = remote(
            halves(ref["full_" + name], half),
            halves(ref["full_" + name], half),
            "join",
            slot,
            (leaf, mate),
        )
        copy.start()
        return copy

    folds = {name: fold_start(name) for name in names[:-1]}
    sent = []
    for k, peer in enumerate(rhs_peers):
        copy = remote(rs_ref, ref["rs"].at[position], "rs", k, (leaf, peer))
        copy.start()
        sent.append(copy)
    ref["rs"][position] = rs_ref[...]
    spreads = {"c0": spread_start("c0", folds["c0"])}

    tile = rank
    order = ord_ref[...]

    def one_hot(i, carry):
        start = pl.multiple_of(i * tile, tile)
        index = lax.broadcasted_iota(jnp.int32, (tile, points), 0) + start
        ref["perm"][pl.ds(start, tile), :] = jnp.where(index == order, 1.0, 0.0).astype(BF16)
        return carry

    lax.fori_loop(0, points // tile, one_hot, 0)
    for name in names[1:-1]:
        spreads[name] = spread_start(name, folds[name])

    for copy in sent:
        copy.wait_recv()
    gathered = ref["rs"][...].reshape(rows, points)
    tree = dot(jnp.concatenate(split(gathered, 3), 0), ref["perm"][...], NN).astype(BF16)
    by_0 = dot(tree, g_parts[0], NN)
    by_1 = dot(tree[: 2 * rows], g_parts[1], NN)
    by_2 = dot(tree[:rows], g_parts[2], NN)
    plain = by_0[:rows] + (
        (by_0[rows : 2 * rows] + by_1[:rows]) + (by_0[2 * rows :] + by_1[rows:] + by_2)
    )
    ref["x"][...] = plain
    term = sum(dot(part, bases_own, NT) for part in reversed(split(plain, 3)))
    for j in range(levels):
        ref["part_t"][j * rows : (j + 1) * rows] = term[:, j * rank : (j + 1) * rank]
    folds["t"] = fold_start("t")

    joins = {"c0": join_start("c0", spreads["c0"])}
    spreads["t"] = spread_start("t", folds["t"])
    eye = (
        lax.broadcasted_iota(jnp.int32, (rank, rank), 0)
        == lax.broadcasted_iota(jnp.int32, (rank, rank), 1)
    ).astype(F32)
    joins["c0"].wait_recv()

    level_copies = {}
    weights = []
    exchanged = []
    for h in range(levels):
        if h == 0:
            capacity = ref["full_c0"][...]
        else:
            level_copies[h, h, 0].wait_recv()
            capacity = ref[f"send{h}_{h}"][:rank] + ref[f"get{h}_{h}"][:rank]
        inverted = inverse(capacity + eye)
        if h == 0:
            for name in names[1:]:
                joins[name] = join_start(name, spreads[name])
            for name in names[1:]:
                joins[name].wait_recv()
            columns = []
            for j in range(levels):
                terms = [ref["full_t"][j * rows : (j + 1) * rows]]
                if f"m{j}" in names:
                    terms = [ref[f"full_m{j}"][...]] + terms
                columns.append(jnp.concatenate(terms, 0))
        else:
            columns = []
            for j in range(h, levels):
                start = rank if j == h else 0
                level_copies[h, j, 1].wait_recv()
                columns.append(ref[f"send{h}_{j}"][start:] + ref[f"get{h}_{j}"][start:])
        rest = columns[0]
        weight = fine(rest, inverted, NN)
        weights.append(weight)
        for j in range(h + 1, levels):
            offset = (j - h - 1) * rank
            update = fine(weight[offset:], rest[offset : offset + rank], NT)
            ref[f"send{h + 1}_{j}"][...] = columns[j - h] - update
            target = (other(leaf, 1 << (h + 1)), position)
            spans = [(1, 0, update.shape[0])]
            if j == h + 1:
                spans = [(0, 0, rank), (1, rank, update.shape[0] - rank)]
            for which, start, count in spans:
                slot = 2 * len(exchanged) + which
                copy = remote(
                    ref[f"send{h + 1}_{j}"].at[pl.ds(start, count)],
                    ref[f"get{h + 1}_{j}"].at[pl.ds(start, count)],
                    "level",
                    slot,
                    target,
                )
                copy.start()
                level_copies[h + 1, j, which] = copy
            exchanged.append((h, j))

    coefficients = [None] * levels
    for h in reversed(range(levels)):
        value = weights[h][(levels - 1 - h) * rank :]
        for j in range(h + 1, levels):
            offset = (j - h - 1) * rank
            value = value - fine(coefficients[j], weights[h][offset : offset + rank], NN)
        coefficients[h] = value
    answer = ref["x"][...] - fine(jnp.concatenate(coefficients, 1), ref["y"][...], NN)
    ref["answer"][...] = answer.reshape(groups, own_rows, piece)
    last = []
    for k, peer in enumerate(rhs_peers):
        copy = remote(ref["answer"].at[peer], ref["final"].at[position], "last", k, (leaf, peer))
        copy.start()
        last.append(copy)
    ref["final"][position] = ref["answer"][position]
    for copy in last:
        copy.wait_recv()
    tree_rows = jnp.concatenate([ref["final"][k] for k in range(groups)], 1)
    moved = dot(jnp.concatenate(split(tree_rows, 3), 0), ref["perm"][...], NT)
    out_ref[...] = moved[:own_rows] + (moved[own_rows : 2 * own_rows] + moved[2 * own_rows :])

    for copy in sent + last + list(folds.values()) + list(joins.values()):
        copy.wait_send()
    for copies in spreads.values():
        for copy in copies:
            copy.wait_send()
    for copy in level_copies.values():
        copy.wait_send()


def scratch_list(cfg):
    leaves, groups, levels, rank, own_rows, points, piece = cfg
    rows = groups * own_rows
    units = plan(leaves, groups, levels, rank, rows)
    chips = groups - 1
    items = [
        ("y", pltpu.VMEM((levels * rank, piece), F32)),
        ("x", pltpu.VMEM((rows, piece), F32)),
        ("rs", pltpu.VMEM((groups, own_rows, points), F32)),
        ("perm", pltpu.VMEM((points, points), BF16)),
        ("answer", pltpu.VMEM((groups, own_rows, piece), F32)),
        ("final", pltpu.VMEM((groups, own_rows, piece), F32)),
    ]
    for name, height in units:
        items += [
            ("part_" + name, pltpu.VMEM((height, rank), F32)),
            ("fold_" + name, pltpu.VMEM((height // 2, rank), F32)),
            ("chip_" + name, pltpu.VMEM((height // 2, rank), F32)),
            ("peer_" + name, pltpu.VMEM((chips, height // 2, rank), F32)),
            ("full_" + name, pltpu.VMEM((height, rank), F32)),
        ]
    pairs = 0
    for h in range(1, levels):
        for j in range(h, levels):
            pairs += 1
            height = (levels - j) * rank + rows
            items.append((f"send{h}_{j}", pltpu.VMEM((height, rank), F32)))
            items.append((f"get{h}_{j}", pltpu.VMEM((height, rank), F32)))
    counts = {
        "rs": groups - 1,
        "last": groups - 1,
        "fold": len(units),
        "join": len(units),
        "peer": len(units) * chips,
        "level": max(1, 2 * pairs),
    }
    for name, count in counts.items():
        items.append((name + "_s", pltpu.SemaphoreType.DMA((count,))))
        items.append((name + "_r", pltpu.SemaphoreType.DMA((count,))))
    return items


def scratch_names(cfg):
    return [name for name, _ in scratch_list(cfg)]


def local(right_sides, leaf_inverse, bases, ordering):
    own_rows, points = right_sides.shape
    levels, rank = bases.shape[:2]
    cfg = (
        lax.axis_size("leaf"),
        lax.axis_size("rhs"),
        levels,
        rank,
        own_rows,
        points,
        leaf_inverse.shape[1],
    )
    return pl.pallas_call(
        functools.partial(kernel, cfg),
        out_shape=jax.ShapeDtypeStruct((own_rows, points), F32),
        in_specs=[pl.BlockSpec(memory_space=pltpu.VMEM)] * 4,
        out_specs=pl.BlockSpec(memory_space=pltpu.VMEM),
        scratch_shapes=[item for _, item in scratch_list(cfg)],
        compiler_params=pltpu.CompilerParams(collective_id=0, has_side_effects=True),
        name="tree_solve",
    )(right_sides, leaf_inverse, bases, ordering)


def solution(mesh):
    placed = (P("rhs", "leaf"), P("leaf", "rhs"), P(None, None, "leaf"), P("leaf", None))
    return jax.shard_map(
        local, mesh=mesh, in_specs=placed, out_specs=P("rhs", "leaf"), check_vma=False
    )
```

```python
import functools

import jax
import jax.numpy as jnp
from jax import lax
from jax.experimental import pallas as pl
from jax.experimental.pallas import tpu as pltpu
from jax.sharding import PartitionSpec as P

F32 = jnp.float32
BF16 = jnp.bfloat16
NN = (((1,), (0,)), ((), ()))
NT = (((1,), (1,)), ((), ()))
STEP = 8


def split(value, pieces):
    parts = []
    for _ in range(pieces):
        head = value.astype(BF16)
        parts.append(head)
        value = value - head.astype(F32)
    return parts


def dot(left, right, dims):
    return lax.dot_general(left, right, dims, preferred_element_type=F32)


def fine(left, right, dims):
    return lax.dot_general(
        left, right, dims, precision=lax.Precision.HIGHEST, preferred_element_type=F32
    )


def inverse(matrix):
    size = matrix.shape[0]
    lane = lax.broadcasted_iota(jnp.int32, (1, size), 1)
    row_of = lax.broadcasted_iota(jnp.int32, (STEP, 1), 0)

    def block(_, a):
        for k in range(0, STEP, 2):
            first, second = a[k : k + 1], a[k + 1 : k + 2]
            a00 = jnp.broadcast_to(a[k : k + 1, k : k + 1], (1, size))
            a01 = jnp.broadcast_to(a[k : k + 1, k + 1 : k + 2], (1, size))
            a10 = jnp.broadcast_to(a[k + 1 : k + 2, k : k + 1], (1, size))
            a11 = jnp.broadcast_to(a[k + 1 : k + 2, k + 1 : k + 2], (1, size))
            scale = 1.0 / (a00 * a11 - a01 * a10)
            at0, at1 = lane == k, lane == k + 1
            first = jnp.where(at0, 1.0, jnp.where(at1, 0.0, first))
            second = jnp.where(at0, 0.0, jnp.where(at1, 1.0, second))
            new0 = (a11 * first - a01 * second) * scale
            new1 = (a00 * second - a10 * first) * scale
            col0, col1 = a[:, k : k + 1], a[:, k + 1 : k + 2]
            kept = jnp.where(at0 | at1, 0.0, a)
            a = kept - col0 * new0 - col1 * new1
            top = jnp.where(row_of == k, new0, jnp.where(row_of == k + 1, new1, a[:STEP]))
            a = jnp.concatenate([top, a[STEP:]], 0)
        a = jnp.concatenate([a[STEP:], a[:STEP]], 0)
        return pltpu.roll(a, size - STEP, 1)

    return lax.fori_loop(0, size // STEP, block, matrix)


def plan(leaves, groups, levels, rank, rows):
    early = [("c0", rank)]
    late = []
    for j in range(levels):
        height = (levels - j) * rank
        if j == 1:
            early.append(("c1", rank))
        if j < 2:
            height -= rank
        if height:
            (late if j else early).append((f"m{j}", height))
    early.append(("t0", rows))
    if levels > 1:
        late.append(("t1", (levels - 1) * rows))
    return early, late


def other(index, bit):
    return index + bit - 2 * bit * ((index // bit) % 2)


def kernel(cfg, rs_ref, g_ref, b_ref, ord_ref, out_ref, *scratch):
    leaves, groups, levels, rank, own_rows, points, piece = cfg
    rows = groups * own_rows
    early, late = plan(leaves, groups, levels, rank, rows)
    early, late = [name for name, _ in early], [name for name, _ in late]
    names = early + late
    ref = dict(zip(scratch_names(cfg), scratch))
    leaf, position = lax.axis_index("leaf"), lax.axis_index("rhs")
    mesh_id = pl.DeviceIdType.MESH

    def at(leaf_index, rhs_index):
        return {"leaf": leaf_index, "rhs": rhs_index}

    rhs_peers = [lax.rem(position + k, groups) for k in range(1, groups)]
    mate = other(position, 1)
    half = lax.rem(position, 2)
    chips = [(leaf, lax.rem(position + k, groups)) for k in range(2, groups, 2)]
    chips += [(other(leaf, 1), lax.rem(position + k, groups)) for k in range(0, groups, 2)]
    greeted = [(leaf, p) for p in rhs_peers]
    greeted += chips[groups // 2 - 1 :]
    greeted += [(other(leaf, 1 << h), position) for h in range(1, levels)]

    barrier = pltpu.get_barrier_semaphore()
    for target in greeted:
        pl.semaphore_signal(barrier, inc=1, device_id=at(*target), device_id_type=mesh_id)

    def remote(src, dst, sems, slot, target):
        return pltpu.make_async_remote_copy(
            src_ref=src,
            dst_ref=dst,
            send_sem=ref[sems + "_s"].at[slot],
            recv_sem=ref[sems + "_r"].at[slot],
            device_id=at(*target),
            device_id_type=mesh_id,
        )

    g_parts = split(g_ref[...], 3)
    for k, part in enumerate(g_parts):
        ref[f"g{k}"][...] = part
    bases = b_ref[...].reshape(levels * rank, points)
    solved = dot(bases, g_parts[0], NN) + (dot(bases, g_parts[1], NN) + dot(bases, g_parts[2], NN))
    ref["y"][...] = solved
    own_cols = pl.ds(pl.multiple_of(position * piece, piece), piece)
    bases_own = b_ref[:, :, own_cols].reshape(levels * rank, piece)
    gram = sum(dot(part, bases_own, NT) for part in reversed(split(solved, 3)))
    for j in range(levels):
        column = gram[j * rank :, j * rank : (j + 1) * rank]
        if j < 2:
            ref[f"part_c{j}"][...] = column[:rank]
            column = column[rank:]
        if column.shape[0]:
            ref[f"part_m{j}"][...] = column

    pl.semaphore_wait(barrier, len(greeted))

    def halves(buffer, which):
        count = buffer.shape[0] // 2
        return buffer.at[pl.ds(pl.multiple_of(which * count, count), count)]

    def fold_start(name):
        slot = names.index(name)
        copy = remote(
            halves(ref["part_" + name], 1 - half), ref["fold_" + name], "fold", slot, (leaf, mate)
        )
        copy.start()
        return copy

    def spread_start(name, fold):
        fold.wait_recv()
        slot = names.index(name)
        ref["chip_" + name][...] = halves(ref["part_" + name], half)[...] + ref["fold_" + name][...]
        copies = []
        for k, target in enumerate(chips):
            copy = remote(
                ref["chip_" + name],
                ref["peer_" + name].at[k],
                "peer",
                slot * len(chips) + k,
                target,
            )
            copy.start()
            copies.append(copy)
        return copies

    def join_start(name, copies):
        for copy in copies:
            copy.wait_recv()
        total = ref["chip_" + name][...]
        for k in range(len(copies)):
            total = total + ref["peer_" + name][k]
        halves(ref["full_" + name], half)[...] = total
        slot = names.index(name)
        copy = remote(
            halves(ref["full_" + name], half),
            halves(ref["full_" + name], half),
            "join",
            slot,
            (leaf, mate),
        )
        copy.start()
        return copy

    grams = [name for name in names if not name.startswith("t")]
    folds = {name: fold_start(name) for name in grams}

    tile = rank
    order = ord_ref[...]

    def one_hot(i, carry):
        start = pl.multiple_of(i * tile, tile)
        index = lax.broadcasted_iota(jnp.int32, (tile, points), 0) + start
        ref["perm"][pl.ds(start, tile), :] = jnp.where(index == order, 1.0, 0.0).astype(BF16)
        return carry

    lax.fori_loop(0, points // tile, one_hot, 0)
    spreads = {"c0": spread_start("c0", folds["c0"])}
    moved = dot(jnp.concatenate(split(rs_ref[...], 3), 0), ref["perm"][...], NN)
    ref["tree"][...] = (moved[:own_rows] + moved[own_rows : 2 * own_rows]) + moved[2 * own_rows :]
    pieces = []
    for k, peer in enumerate(rhs_peers):
        copy = remote(
            ref["tree"].at[:, pl.ds(pl.multiple_of(peer * piece, piece), piece)],
            ref["cols"].at[position],
            "cols",
            k,
            (leaf, peer),
        )
        copy.start()
        pieces.append(copy)
    ref["cols"][position] = ref["tree"][:, own_cols]
    for name in early[1:]:
        if name in grams:
            spreads[name] = spread_start(name, folds[name])
    for copy in pieces:
        copy.wait_recv()
    term = fine(ref["cols"][...].reshape(rows, piece), ref["y"][...], NT)
    ref["part_t0"][...] = term[:, :rank]
    folds["t0"] = fold_start("t0")
    for j in range(1, levels):
        ref["part_t1"][(j - 1) * rows : j * rows] = term[:, j * rank : (j + 1) * rank]
    if levels > 1:
        folds["t1"] = fold_start("t1")
    spreads["t0"] = spread_start("t0", folds["t0"])
    for name in late:
        spreads[name] = spread_start(name, folds[name])
    sent = []
    for k, peer in enumerate(rhs_peers):
        copy = remote(ref["tree"], ref["rs"].at[position], "rs", k, (leaf, peer))
        copy.start()
        sent.append(copy)
    ref["rs"][position] = ref["tree"][...]

    def plain_term():
        for copy in sent:
            copy.wait_recv()
        gathered = ref["rs"][...].reshape(rows, points)
        stack = jnp.concatenate(split(gathered, 3), 0)
        by_0 = dot(stack, ref["g0"][...], NN)
        by_1 = dot(stack[: 2 * rows], ref["g1"][...], NN)
        by_2 = dot(stack[:rows], ref["g2"][...], NN)
        ref["x"][...] = by_0[:rows] + (
            (by_0[rows : 2 * rows] + by_1[:rows]) + (by_0[2 * rows :] + by_1[rows:] + by_2)
        )

    joins = {"c0": join_start("c0", spreads["c0"])}
    eye = (
        lax.broadcasted_iota(jnp.int32, (rank, rank), 0)
        == lax.broadcasted_iota(jnp.int32, (rank, rank), 1)
    ).astype(F32)
    joins["c0"].wait_recv()

    level_copies = {}
    weights = []
    slots = iter(range(levels * levels * 2))

    def level_start(h, j, which, start, value):
        span = pl.ds(start, value.shape[0])
        ref[f"send{h}_{j}"][span, :] = value
        copy = remote(
            ref[f"send{h}_{j}"].at[span],
            ref[f"get{h}_{j}"].at[span],
            "level",
            next(slots),
            (other(leaf, 1 << h), position),
        )
        copy.start()
        level_copies[h, j, which] = copy

    def level_value(h, j, start):
        return ref[f"send{h}_{j}"][start:] + ref[f"get{h}_{j}"][start:]

    for h in range(levels):
        if h == 0:
            capacity = ref["full_c0"][...]
        else:
            level_copies[h, h, 0].wait_recv()
            capacity = ref[f"send{h}_{h}"][:rank] + ref[f"get{h}_{h}"][:rank]
        inverted = inverse(capacity + eye)
        if h == 0:
            for name in early[1:]:
                joins[name] = join_start(name, spreads[name])
            for name in early[1:]:
                joins[name].wait_recv()
            rest = ref["full_t0"][...]
            if levels > 1:
                rest = jnp.concatenate([ref["full_m0"][...], rest], 0)
                head = ref["full_c1"][...]
        else:
            level_copies[h, h, 1].wait_recv()
            rest = level_value(h, h, rank)
            if h + 1 < levels:
                level_copies[h, h + 1, 1].wait_recv()
                following = level_value(h, h + 1, 0)
                head, tail = following[:rank], following[rank:]
        if h + 1 < levels:
            first = fine(rest[:rank], inverted, NN)
            level_start(h + 1, h + 1, 0, 0, head - fine(first, rest[:rank], NT))
            weight = jnp.concatenate([first, fine(rest[rank:], inverted, NN)], 0)
        else:
            weight = fine(rest, inverted, NN)
        weights.append(weight)
        if h == 0:
            for name in late:
                joins[name] = join_start(name, spreads[name])
            for name in late:
                joins[name].wait_recv()
        for j in range(h + 1, levels):
            offset = (j - h - 1) * rank
            start = rank if j == h + 1 else 0
            if h == 0:
                column = ref["full_t1"][(j - 1) * rows : j * rows]
                if f"m{j}" in names:
                    column = jnp.concatenate([ref[f"full_m{j}"][...], column], 0)
            elif j == h + 1:
                column = tail
            else:
                level_copies[h, j, 1].wait_recv()
                column = level_value(h, j, 0)
            update = fine(weight[offset + start :], rest[offset : offset + rank], NT)
            level_start(h + 1, j, 1, start, column - update)
        if h == max(levels - 2, 0):
            plain_term()

    coefficients = [None] * levels
    for h in reversed(range(levels)):
        value = weights[h][(levels - 1 - h) * rank :]
        for j in range(h + 1, levels):
            offset = (j - h - 1) * rank
            value = value - fine(coefficients[j], weights[h][offset : offset + rank], NN)
        coefficients[h] = value
    answer = ref["x"][...] - fine(jnp.concatenate(coefficients, 1), ref["y"][...], NN)
    ref["answer"][...] = answer.reshape(groups, own_rows, piece)
    last = []
    for k, peer in enumerate(rhs_peers):
        copy = remote(ref["answer"].at[peer], ref["final"].at[position], "last", k, (leaf, peer))
        copy.start()
        last.append(copy)
    ref["final"][position] = ref["answer"][position]
    for copy in last:
        copy.wait_recv()
    tree_rows = jnp.concatenate([ref["final"][k] for k in range(groups)], 1)
    moved = dot(jnp.concatenate(split(tree_rows, 3), 0), ref["perm"][...], NT)
    out_ref[...] = moved[:own_rows] + (moved[own_rows : 2 * own_rows] + moved[2 * own_rows :])

    for copy in pieces + sent + last + list(folds.values()) + list(joins.values()):
        copy.wait_send()
    for copies in spreads.values():
        for copy in copies:
            copy.wait_send()
    for copy in level_copies.values():
        copy.wait_send()


def scratch_list(cfg):
    leaves, groups, levels, rank, own_rows, points, piece = cfg
    rows = groups * own_rows
    early, late = plan(leaves, groups, levels, rank, rows)
    units = early + late
    chips = groups - 1
    items = [
        ("y", pltpu.VMEM((levels * rank, piece), F32)),
        ("x", pltpu.VMEM((rows, piece), F32)),
        ("rs", pltpu.VMEM((groups, own_rows, points), F32)),
        ("tree", pltpu.VMEM((own_rows, points), F32)),
        ("cols", pltpu.VMEM((groups, own_rows, piece), F32)),
        ("g0", pltpu.VMEM((points, piece), BF16)),
        ("g1", pltpu.VMEM((points, piece), BF16)),
        ("g2", pltpu.VMEM((points, piece), BF16)),
        ("perm", pltpu.VMEM((points, points), BF16)),
        ("answer", pltpu.VMEM((groups, own_rows, piece), F32)),
        ("final", pltpu.VMEM((groups, own_rows, piece), F32)),
    ]
    for name, height in units:
        items += [
            ("part_" + name, pltpu.VMEM((height, rank), F32)),
            ("fold_" + name, pltpu.VMEM((height // 2, rank), F32)),
            ("chip_" + name, pltpu.VMEM((height // 2, rank), F32)),
            ("peer_" + name, pltpu.VMEM((chips, height // 2, rank), F32)),
            ("full_" + name, pltpu.VMEM((height, rank), F32)),
        ]
    pairs = 0
    for h in range(1, levels):
        for j in range(h, levels):
            pairs += 1
            height = (levels - j) * rank + rows
            items.append((f"send{h}_{j}", pltpu.VMEM((height, rank), F32)))
            items.append((f"get{h}_{j}", pltpu.VMEM((height, rank), F32)))
    counts = {
        "rs": groups - 1,
        "cols": groups - 1,
        "last": groups - 1,
        "fold": len(units),
        "join": len(units),
        "peer": len(units) * chips,
        "level": max(1, 2 * pairs),
    }
    for name, count in counts.items():
        items.append((name + "_s", pltpu.SemaphoreType.DMA((count,))))
        items.append((name + "_r", pltpu.SemaphoreType.DMA((count,))))
    return items


def scratch_names(cfg):
    return [name for name, _ in scratch_list(cfg)]


def local(right_sides, leaf_inverse, bases, ordering):
    own_rows, points = right_sides.shape
    levels, rank = bases.shape[:2]
    cfg = (
        lax.axis_size("leaf"),
        lax.axis_size("rhs"),
        levels,
        rank,
        own_rows,
        points,
        leaf_inverse.shape[1],
    )
    return pl.pallas_call(
        functools.partial(kernel, cfg),
        out_shape=jax.ShapeDtypeStruct((own_rows, points), F32),
        in_specs=[pl.BlockSpec(memory_space=pltpu.VMEM)] * 4,
        out_specs=pl.BlockSpec(memory_space=pltpu.VMEM),
        scratch_shapes=[item for _, item in scratch_list(cfg)],
        compiler_params=pltpu.CompilerParams(collective_id=0, has_side_effects=True),
        name="tree_solve",
    )(right_sides, leaf_inverse, bases, ordering)


def solution(mesh):
    placed = (P("rhs", "leaf"), P("leaf", "rhs"), P(None, None, "leaf"), P("leaf", None))
    return jax.shard_map(
        local, mesh=mesh, in_specs=placed, out_specs=P("rhs", "leaf"), check_vma=False
    )
```

```python
import functools

import jax
import jax.numpy as jnp
from jax import lax
from jax.experimental import pallas as pl
from jax.experimental.pallas import tpu as pltpu
from jax.sharding import PartitionSpec as P

F32 = jnp.float32
BF16 = jnp.bfloat16
NN = (((1,), (0,)), ((), ()))
NT = (((1,), (1,)), ((), ()))
STEP = 32
TILE = 8


def split(value, pieces):
    parts = []
    for _ in range(pieces):
        head = value.astype(BF16)
        parts.append(head)
        value = value - head.astype(F32)
    return parts


def dot(left, right, dims):
    return lax.dot_general(left, right, dims, preferred_element_type=F32)


def fine(left, right, dims):
    return lax.dot_general(
        left, right, dims, precision=lax.Precision.HIGHEST, preferred_element_type=F32
    )


def inverse(matrix):
    size = matrix.shape[0]
    lane = lax.broadcasted_iota(jnp.int32, (1, size), 1)
    row_of = lax.broadcasted_iota(jnp.int32, (TILE, 1), 0)

    def block(_, a):
        for k in range(0, STEP, 2):
            first, second = a[k : k + 1], a[k + 1 : k + 2]
            a00 = jnp.broadcast_to(a[k : k + 1, k : k + 1], (1, size))
            a01 = jnp.broadcast_to(a[k : k + 1, k + 1 : k + 2], (1, size))
            a10 = jnp.broadcast_to(a[k + 1 : k + 2, k : k + 1], (1, size))
            a11 = jnp.broadcast_to(a[k + 1 : k + 2, k + 1 : k + 2], (1, size))
            scale = 1.0 / (a00 * a11 - a01 * a10)
            at0, at1 = lane == k, lane == k + 1
            first = jnp.where(at0, 1.0, jnp.where(at1, 0.0, first))
            second = jnp.where(at0, 0.0, jnp.where(at1, 1.0, second))
            new0 = (a11 * first - a01 * second) * scale
            new1 = (a00 * second - a10 * first) * scale
            col0, col1 = a[:, k : k + 1], a[:, k + 1 : k + 2]
            kept = jnp.where(at0 | at1, 0.0, a)
            a = kept - col0 * new0 - col1 * new1
            base = k // TILE * TILE
            rows = a[base : base + TILE]
            rows = jnp.where(row_of == k - base, new0, rows)
            rows = jnp.where(row_of == k + 1 - base, new1, rows)
            before = [a[:base]] if base else []
            a = jnp.concatenate(before + [rows, a[base + TILE :]], 0)
        a = jnp.concatenate([a[STEP:], a[:STEP]], 0)
        return pltpu.roll(a, size - STEP, 1)

    return lax.fori_loop(0, size // STEP, block, matrix)


def plan(leaves, groups, levels, rank, rows):
    early = [("c0", rank)]
    late = []
    for j in range(levels):
        height = (levels - j) * rank
        if j == 1:
            early.append(("c1", rank))
        if j < 2:
            height -= rank
        if height:
            (late if j else early).append((f"m{j}", height))
    early.append(("t0", rows))
    if levels > 1:
        late.append(("t1", (levels - 1) * rows))
    return early, late


def other(index, bit):
    return index + bit - 2 * bit * ((index // bit) % 2)


def kernel(cfg, rs_ref, g_ref, b_ref, ord_ref, out_ref, *scratch):
    leaves, groups, levels, rank, own_rows, points, piece = cfg
    rows = groups * own_rows
    early, late = plan(leaves, groups, levels, rank, rows)
    early, late = [name for name, _ in early], [name for name, _ in late]
    names = early + late
    ref = dict(zip(scratch_names(cfg), scratch))
    leaf, position = lax.axis_index("leaf"), lax.axis_index("rhs")
    mesh_id = pl.DeviceIdType.MESH

    def at(leaf_index, rhs_index):
        return {"leaf": leaf_index, "rhs": rhs_index}

    rhs_peers = [lax.rem(position + k, groups) for k in range(1, groups)]
    mate = other(position, 1)
    half = lax.rem(position, 2)
    chips = [(leaf, lax.rem(position + k, groups)) for k in range(2, groups, 2)]
    chips += [(other(leaf, 1), lax.rem(position + k, groups)) for k in range(0, groups, 2)]
    greeted = [(leaf, p) for p in rhs_peers]
    greeted += chips[groups // 2 - 1 :]
    greeted += [(other(leaf, 1 << h), position) for h in range(1, levels)]

    barrier = pltpu.get_barrier_semaphore()
    for target in greeted:
        pl.semaphore_signal(barrier, inc=1, device_id=at(*target), device_id_type=mesh_id)

    def remote(src, dst, sems, slot, target):
        return pltpu.make_async_remote_copy(
            src_ref=src,
            dst_ref=dst,
            send_sem=ref[sems + "_s"].at[slot],
            recv_sem=ref[sems + "_r"].at[slot],
            device_id=at(*target),
            device_id_type=mesh_id,
        )

    g_parts = split(g_ref[...], 3)
    for k, part in enumerate(g_parts):
        ref[f"g{k}"][...] = part
    bases = b_ref[...].reshape(levels * rank, points)
    solved = dot(bases, g_parts[0], NN) + (dot(bases, g_parts[1], NN) + dot(bases, g_parts[2], NN))
    ref["y"][...] = solved
    own_cols = pl.ds(pl.multiple_of(position * piece, piece), piece)
    bases_own = b_ref[:, :, own_cols].reshape(levels * rank, piece)
    gram = sum(dot(part, bases_own, NT) for part in reversed(split(solved, 3)))
    for j in range(levels):
        column = gram[j * rank :, j * rank : (j + 1) * rank]
        if j < 2:
            ref[f"part_c{j}"][...] = column[:rank]
            column = column[rank:]
        if column.shape[0]:
            ref[f"part_m{j}"][...] = column

    pl.semaphore_wait(barrier, len(greeted))

    def halves(buffer, which):
        count = buffer.shape[0] // 2
        return buffer.at[pl.ds(pl.multiple_of(which * count, count), count)]

    def fold_start(name):
        slot = names.index(name)
        copy = remote(
            halves(ref["part_" + name], 1 - half), ref["fold_" + name], "fold", slot, (leaf, mate)
        )
        copy.start()
        return copy

    def spread_start(name, fold):
        fold.wait_recv()
        slot = names.index(name)
        ref["chip_" + name][...] = halves(ref["part_" + name], half)[...] + ref["fold_" + name][...]
        copies = []
        for k, target in enumerate(chips):
            copy = remote(
                ref["chip_" + name],
                ref["peer_" + name].at[k],
                "peer",
                slot * len(chips) + k,
                target,
            )
            copy.start()
            copies.append(copy)
        return copies

    def join_start(name, copies):
        for copy in copies:
            copy.wait_recv()
        total = ref["chip_" + name][...]
        for k in range(len(copies)):
            total = total + ref["peer_" + name][k]
        halves(ref["full_" + name], half)[...] = total
        slot = names.index(name)
        copy = remote(
            halves(ref["full_" + name], half),
            halves(ref["full_" + name], half),
            "join",
            slot,
            (leaf, mate),
        )
        copy.start()
        return copy

    grams = [name for name in names if not name.startswith("t")]
    folds = {name: fold_start(name) for name in grams}

    tile = rank
    order = ord_ref[...]

    def one_hot(i, carry):
        start = pl.multiple_of(i * tile, tile)
        index = lax.broadcasted_iota(jnp.int32, (tile, points), 0) + start
        ref["perm"][pl.ds(start, tile), :] = jnp.where(index == order, 1.0, 0.0).astype(BF16)
        return carry

    lax.fori_loop(0, points // tile, one_hot, 0)
    spreads = {"c0": spread_start("c0", folds["c0"])}
    moved = dot(jnp.concatenate(split(rs_ref[...], 3), 0), ref["perm"][...], NN)
    ref["tree"][...] = (moved[:own_rows] + moved[own_rows : 2 * own_rows]) + moved[2 * own_rows :]
    pieces = []
    for k, peer in enumerate(rhs_peers):
        copy = remote(
            ref["tree"].at[:, pl.ds(pl.multiple_of(peer * piece, piece), piece)],
            ref["cols"].at[position],
            "cols",
            k,
            (leaf, peer),
        )
        copy.start()
        pieces.append(copy)
    ref["cols"][position] = ref["tree"][:, own_cols]
    for name in early[1:]:
        if name in grams:
            spreads[name] = spread_start(name, folds[name])
    for copy in pieces:
        copy.wait_recv()
    term = fine(ref["cols"][...].reshape(rows, piece), ref["y"][...], NT)
    ref["part_t0"][...] = term[:, :rank]
    folds["t0"] = fold_start("t0")
    for j in range(1, levels):
        ref["part_t1"][(j - 1) * rows : j * rows] = term[:, j * rank : (j + 1) * rank]
    if levels > 1:
        folds["t1"] = fold_start("t1")
    spreads["t0"] = spread_start("t0", folds["t0"])
    for name in late:
        spreads[name] = spread_start(name, folds[name])
    sent = []
    for k, peer in enumerate(rhs_peers):
        copy = remote(ref["tree"], ref["rs"].at[position], "rs", k, (leaf, peer))
        copy.start()
        sent.append(copy)
    ref["rs"][position] = ref["tree"][...]

    def plain_term():
        for copy in sent:
            copy.wait_recv()
        gathered = ref["rs"][...].reshape(rows, points)
        stack = jnp.concatenate(split(gathered, 3), 0)
        by_0 = dot(stack, ref["g0"][...], NN)
        by_1 = dot(stack[: 2 * rows], ref["g1"][...], NN)
        by_2 = dot(stack[:rows], ref["g2"][...], NN)
        ref["x"][...] = by_0[:rows] + (
            (by_0[rows : 2 * rows] + by_1[:rows]) + (by_0[2 * rows :] + by_1[rows:] + by_2)
        )

    joins = {"c0": join_start("c0", spreads["c0"])}
    eye = (
        lax.broadcasted_iota(jnp.int32, (rank, rank), 0)
        == lax.broadcasted_iota(jnp.int32, (rank, rank), 1)
    ).astype(F32)
    joins["c0"].wait_recv()

    level_copies = {}
    weights = []
    slots = iter(range(levels * levels * 2))

    def level_start(h, j, which, start, value):
        span = pl.ds(start, value.shape[0])
        ref[f"send{h}_{j}"][span, :] = value
        copy = remote(
            ref[f"send{h}_{j}"].at[span],
            ref[f"get{h}_{j}"].at[span],
            "level",
            next(slots),
            (other(leaf, 1 << h), position),
        )
        copy.start()
        level_copies[h, j, which] = copy

    def level_value(h, j, start):
        return ref[f"send{h}_{j}"][start:] + ref[f"get{h}_{j}"][start:]

    for h in range(levels):
        if h == 0:
            capacity = ref["full_c0"][...]
        else:
            level_copies[h, h, 0].wait_recv()
            capacity = ref[f"send{h}_{h}"][:rank] + ref[f"get{h}_{h}"][:rank]
        inverted = inverse(capacity + eye)
        if h == 0:
            for name in early[1:]:
                joins[name] = join_start(name, spreads[name])
            for name in early[1:]:
                joins[name].wait_recv()
            rest = ref["full_t0"][...]
            if levels > 1:
                rest = jnp.concatenate([ref["full_m0"][...], rest], 0)
                head = ref["full_c1"][...]
        else:
            level_copies[h, h, 1].wait_recv()
            rest = level_value(h, h, rank)
            if h + 1 < levels:
                level_copies[h, h + 1, 1].wait_recv()
                following = level_value(h, h + 1, 0)
                head, tail = following[:rank], following[rank:]
        if h + 1 < levels:
            first = fine(rest[:rank], inverted, NN)
            level_start(h + 1, h + 1, 0, 0, head - fine(first, rest[:rank], NT))
            weight = jnp.concatenate([first, fine(rest[rank:], inverted, NN)], 0)
        else:
            weight = fine(rest, inverted, NN)
        weights.append(weight)
        if h == 0:
            for name in late:
                joins[name] = join_start(name, spreads[name])
            for name in late:
                joins[name].wait_recv()
        for j in range(h + 1, levels):
            offset = (j - h - 1) * rank
            start = rank if j == h + 1 else 0
            if h == 0:
                column = ref["full_t1"][(j - 1) * rows : j * rows]
                if f"m{j}" in names:
                    column = jnp.concatenate([ref[f"full_m{j}"][...], column], 0)
            elif j == h + 1:
                column = tail
            else:
                level_copies[h, j, 1].wait_recv()
                column = level_value(h, j, 0)
            update = fine(weight[offset + start :], rest[offset : offset + rank], NT)
            level_start(h + 1, j, 1, start, column - update)
        if h == max(levels - 2, 0):
            plain_term()

    coefficients = [None] * levels
    for h in reversed(range(levels)):
        value = weights[h][(levels - 1 - h) * rank :]
        for j in range(h + 1, levels):
            offset = (j - h - 1) * rank
            value = value - fine(coefficients[j], weights[h][offset : offset + rank], NN)
        coefficients[h] = value
    answer = ref["x"][...] - fine(jnp.concatenate(coefficients, 1), ref["y"][...], NN)
    ref["answer"][...] = answer.reshape(groups, own_rows, piece)
    last = []
    for k, peer in enumerate(rhs_peers):
        copy = remote(ref["answer"].at[peer], ref["final"].at[position], "last", k, (leaf, peer))
        copy.start()
        last.append(copy)
    ref["final"][position] = ref["answer"][position]
    for copy in last:
        copy.wait_recv()
    tree_rows = jnp.concatenate([ref["final"][k] for k in range(groups)], 1)
    moved = dot(jnp.concatenate(split(tree_rows, 3), 0), ref["perm"][...], NT)
    out_ref[...] = moved[:own_rows] + (moved[own_rows : 2 * own_rows] + moved[2 * own_rows :])

    for copy in pieces + sent + last + list(folds.values()) + list(joins.values()):
        copy.wait_send()
    for copies in spreads.values():
        for copy in copies:
            copy.wait_send()
    for copy in level_copies.values():
        copy.wait_send()


def scratch_list(cfg):
    leaves, groups, levels, rank, own_rows, points, piece = cfg
    rows = groups * own_rows
    early, late = plan(leaves, groups, levels, rank, rows)
    units = early + late
    chips = groups - 1
    items = [
        ("y", pltpu.VMEM((levels * rank, piece), F32)),
        ("x", pltpu.VMEM((rows, piece), F32)),
        ("rs", pltpu.VMEM((groups, own_rows, points), F32)),
        ("tree", pltpu.VMEM((own_rows, points), F32)),
        ("cols", pltpu.VMEM((groups, own_rows, piece), F32)),
        ("g0", pltpu.VMEM((points, piece), BF16)),
        ("g1", pltpu.VMEM((points, piece), BF16)),
        ("g2", pltpu.VMEM((points, piece), BF16)),
        ("perm", pltpu.VMEM((points, points), BF16)),
        ("answer", pltpu.VMEM((groups, own_rows, piece), F32)),
        ("final", pltpu.VMEM((groups, own_rows, piece), F32)),
    ]
    for name, height in units:
        items += [
            ("part_" + name, pltpu.VMEM((height, rank), F32)),
            ("fold_" + name, pltpu.VMEM((height // 2, rank), F32)),
            ("chip_" + name, pltpu.VMEM((height // 2, rank), F32)),
            ("peer_" + name, pltpu.VMEM((chips, height // 2, rank), F32)),
            ("full_" + name, pltpu.VMEM((height, rank), F32)),
        ]
    pairs = 0
    for h in range(1, levels):
        for j in range(h, levels):
            pairs += 1
            height = (levels - j) * rank + rows
            items.append((f"send{h}_{j}", pltpu.VMEM((height, rank), F32)))
            items.append((f"get{h}_{j}", pltpu.VMEM((height, rank), F32)))
    counts = {
        "rs": groups - 1,
        "cols": groups - 1,
        "last": groups - 1,
        "fold": len(units),
        "join": len(units),
        "peer": len(units) * chips,
        "level": max(1, 2 * pairs),
    }
    for name, count in counts.items():
        items.append((name + "_s", pltpu.SemaphoreType.DMA((count,))))
        items.append((name + "_r", pltpu.SemaphoreType.DMA((count,))))
    return items


def scratch_names(cfg):
    return [name for name, _ in scratch_list(cfg)]


def local(right_sides, leaf_inverse, bases, ordering):
    own_rows, points = right_sides.shape
    levels, rank = bases.shape[:2]
    cfg = (
        lax.axis_size("leaf"),
        lax.axis_size("rhs"),
        levels,
        rank,
        own_rows,
        points,
        leaf_inverse.shape[1],
    )
    return pl.pallas_call(
        functools.partial(kernel, cfg),
        out_shape=jax.ShapeDtypeStruct((own_rows, points), F32),
        in_specs=[pl.BlockSpec(memory_space=pltpu.VMEM)] * 4,
        out_specs=pl.BlockSpec(memory_space=pltpu.VMEM),
        scratch_shapes=[item for _, item in scratch_list(cfg)],
        compiler_params=pltpu.CompilerParams(collective_id=0, has_side_effects=True),
        name="tree_solve",
    )(right_sides, leaf_inverse, bases, ordering)


def solution(mesh):
    placed = (P("rhs", "leaf"), P("leaf", "rhs"), P(None, None, "leaf"), P("leaf", None))
    return jax.shard_map(
        local, mesh=mesh, in_specs=placed, out_specs=P("rhs", "leaf"), check_vma=False
    )
```
